256 devices in a mesh: gx: 8 (over z_hi, y), gy: 8 (over z_lo, core), gz: 4 (over x).
Axes of the slice: x: 4, y: 4, z: 8 (z_hi: 2, z_lo: 4; z = z_hi * 4 + z_lo), core: 2. Of those that a mesh axis runs over, the one named last changes fastest.
Arguments:
- concentration: float32 [128, 512, 512], P('gx', 'gy', 'gz'), may hold values from -6 to 6
- speed: float32 [3, 128, 512, 512], P(None, 'gx', 'gy', 'gz'), may hold values from 0.1 to 1
- signs: int32 [3, 128, 512, 512], P(None, 'gx', 'gy', 'gz'), may hold values from 0 to 1
- diffusivity: float32 [128, 512, 512], P('gx', 'gy', 'gz'), may hold values from 0.02 to 0.12
- shear: int32 [1], replicated, may hold values from 0 to 511
Outputs:
- final_field: float32 [128, 512, 512], P('gx', 'gy', 'gz')
The draws below stay inside these ranges and needn't reach their ends.
All inputs are finite; a program needn't handle non-finite values.
Results may differ from the reference program's by a relative error of at most 0.00002.
Values sent between devices are 32-bit elements; how exact they have to be, the bound alone decides.
A program may use at most 64 MiB of HBM per device.

```python
import math
import jax
import jax.numpy as jnp

STEPS = 8
NX = 128
NY = 512
NZ = 512


def with_ends(values, rng, low, largest):
    shape = values.shape
    place = [jax.random.randint(jax.random.fold_in(rng, axis), (), 0, shape[axis]) for axis in range(len(shape))]
    values = values.at[tuple(place)].set(low)
    longest = shape.index(max(shape))
    place[longest] = (place[longest] + 1) % shape[longest]
    return values.at[tuple(place)].set(largest)


def level_of(rng, shape, shards, least, high):
    loudness, own = 1.0, jax.random.fold_in(rng, 6)
    for position, parts in shards:
        draws = jnp.exp(jax.random.uniform(jax.random.fold_in(own, position), (parts,), jnp.float32, least / len(shards), high / len(shards)))
        loudness = loudness * jnp.repeat(draws, shape[position] // parts).reshape([-1 if axis == position else 1 for axis in range(len(shape))])
    return loudness


def scatter_about(own_key, dims, width, limit, pieces=(), kind=jnp.bfloat16):
    entries = width * jax.random.normal(own_key, dims, jnp.float32)
    if pieces:
        entries = entries * level_of(own_key, dims, pieces, -0.22, 0.18)
    return jnp.clip(entries, -limit, limit).astype(kind)


def setup_inputs(seed: int = 0) -> dict:
    key_list = jax.random.split(jax.random.key(seed), 6)
    concentration = scatter_about(key_list[0], (NX, NY, NZ), 1.0, 6.0, ((0, 8), (1, 8), (2, 4)), jnp.float32)
    speed = jnp.clip(jnp.exp(math.log(1.0) - 2.3025851 * jax.random.uniform(key_list[1], (3, NX, NY, NZ), jnp.float32) ** level_of(key_list[1], (3, NX, NY, NZ), ((1, 8), (2, 8), (3, 4)), -0.2, 0.2)), 0.1, 1.0)
    signs = with_ends(jax.random.randint(key_list[2], (3, NX, NY, NZ), 0, 2), jax.random.fold_in(key_list[2], 1), 0, 1).astype(jnp.int32)
    diffusivity = jnp.clip(jnp.exp(math.log(0.12) - 1.7917595 * jax.random.uniform(key_list[3], (NX, NY, NZ), jnp.float32) ** level_of(key_list[3], (NX, NY, NZ), ((0, 8), (1, 8), (2, 4)), -0.2, 0.2)), 0.02, 0.12)
    shear = jax.random.randint(key_list[4], (1,), 0, NY).astype(jnp.int32)
    return {"concentration": concentration, "speed": speed, "signs": signs, "diffusivity": diffusivity, "shear": shear}


time_step = 0.25


def advance(field, neighbours, speed, signs, diffusivity):
    total = jnp.zeros_like(field)
    for axis_id in range(3):
        below, above = neighbours[axis_id]
        upwind = jnp.where(signs[axis_id] > 0, field - below, above - field)
        total = total + diffusivity * (above + below - 2.0 * field) - speed[axis_id] * upwind
    return field + time_step * total


def reference(concentration, speed, signs, diffusivity, shear):
    offset = shear[0]
    field = concentration
    for step in range(STEPS):
        lower = jnp.roll(field[-1], -offset, axis=0)
        upper = jnp.roll(field[0], offset, axis=0)
        x_minus = jnp.concatenate([lower[None], field[:-1]], axis=0)
        x_plus = jnp.concatenate([field[1:], upper[None]], axis=0)
        y_minus = jnp.roll(field, 1, axis=1)
        y_plus = jnp.roll(field, -1, axis=1)
        z_minus = jnp.roll(field, 1, axis=2)
        z_plus = jnp.roll(field, -1, axis=2)
        field = advance(field, ((x_minus, x_plus), (y_minus, y_plus), (z_minus, z_plus)), speed, signs, diffusivity)
    return field
```

```python
import functools

import jax
import jax.numpy as jnp
from jax import lax
from jax.experimental import pallas as pl
from jax.experimental.pallas import tpu as pltpu
from jax.sharding import PartitionSpec as P

STEPS = 8
DT = 0.25
MESH = pl.DeviceIdType.MESH


def coefficients(diffusivity, velocities):
    base = DT * diffusivity
    sides = []
    for velocity in velocities:
        sides.append(base + DT * jnp.maximum(velocity, 0.0))
        sides.append(base + DT * jnp.minimum(velocity, 0.0))
    own = 1.0
    for side in sides:
        own = own - side
    return [own] + sides


def weigh(weights, cells):
    total = weights[0] * cells[0]
    for weight, cell in zip(weights[1:], cells[1:]):
        total = total + weight * cell
    return total


def kernel(q, sizes, r_ref, conc, speed, signs, diff, out, F, T, F1, T1, C, CT, CY, S, SPD, SGN, SB, LB, ST, XZS, XZR,
           YS, YR, YZR, ZS, ZR, CXR, CYS, CYR, CZS, CZR, load_sem, send_sem, recv_sem, csend_sem, crecv_sem, out_sem):
    nx, ny, nz = sizes
    X, Y, Z = 16, 64, 128
    tiles = Y // 8
    rounds = STEPS // 2
    gx, gy, gz = lax.axis_index("gx"), lax.axis_index("gy"), lax.axis_index("gz")
    lane = lax.broadcasted_iota(jnp.int32, (8, Z), 1)
    l0, l127, from_left = lane == 0, lane == Z - 1, (lane & 2) == 0
    lane16 = lax.broadcasted_iota(jnp.int32, (X, Z), 1)
    first16, last16, low16 = lane16 == 0, lane16 == Z - 1, lane16 < 64
    r = r_ref[0]
    slide = (gx == nx - 1, gx == 0)
    recv_slide = (gx == 0, gx == nx - 1)
    start = (jnp.where(recv_slide[0], r, 0), jnp.where(recv_slide[1], 64 - r, 64))

    def wrap(value, n):
        return lax.rem(value + 2 * n, n)

    def x_targets(d):
        sign = 1 if d == 0 else -1
        to = wrap(gx + sign, nx)
        shift = jnp.where(slide[d], q, 0) * sign
        return to, wrap(gy - shift, ny), wrap(gy - shift - sign, ny), wrap(gy - shift + sign, ny)

    zs = ((1, 0), (-1, 1))

    def x_messages(par):
        found = []
        for d in range(2):
            to, at_a, at_n, at_e = x_targets(d)
            yes, no = slide[d], jnp.logical_not(slide[d])
            ryes, rno = recv_slide[d], jnp.logical_not(recv_slide[d])
            planes = F.at[pl.ds(X, 2), pl.ds(8, Y)] if d == 0 else F.at[pl.ds(2, 2), pl.ds(8, Y)]
            near, near_slot = (X + 1, 1) if d == 0 else (2, 0)
            first, last = F.at[near, pl.ds(8, 8)], F.at[near, pl.ds(Y, 8)]
            a_row, n_row = (8, 72) if d == 0 else (72, 8)
            found.append((d, None, None, planes, SB.at[par, d, :, pl.ds(a_row, Y)], (to, at_a, gz)))
            found.append((2 + d, yes, ryes, planes, SB.at[par, d, :, pl.ds(n_row, Y)], (to, at_n, gz)))
            if d == 0:
                found.append((2 + d, no, rno, first, SB.at[par, d, near_slot, pl.ds(72, 8)], (to, at_n, gz)))
                found.append((4 + d, None, None, last, SB.at[par, d, near_slot, pl.ds(0, 8)], (to, at_e, gz)))
            else:
                found.append((2 + d, no, rno, last, SB.at[par, d, near_slot, pl.ds(64, 8)], (to, at_n, gz)))
                found.append((4 + d, None, None, first, SB.at[par, d, near_slot, pl.ds(136, 8)], (to, at_e, gz)))
            for step, slot in zs:
                side = wrap(gz + step, nz)
                found.append((6 + 2 * d + slot, None, None, XZS.at[d], XZR.at[par, d, 0, slot], (to, at_a, side)))
                found.append((10 + 2 * d + slot, yes, ryes, XZS.at[d], XZR.at[par, d, 1, slot], (to, at_n, side)))
        return found

    def yz_messages(par):
        found = []
        for d in range(2):
            to = wrap(gy + 1 - 2 * d, ny)
            found.append((14 + d, None, None, YS.at[d], YR.at[par, d], (gx, to, gz)))
            for step, slot in zs:
                found.append((18 + 2 * d + slot, None, None, YS.at[d, 0], YZR.at[par, d, slot],
                              (gx, to, wrap(gz + step, nz))))
        for step, slot in zs:
            found.append((16 + slot, None, None, ZS, ZR.at[par, slot], (gx, gy, wrap(gz + step, nz))))
        return found

    def cx_messages():
        found = []
        for d in range(2):
            to, at_a, at_n, _ = x_targets(d)
            a_row, n_row = (8, 72) if d == 0 else (72, 8)
            plane = S.at[:, X - 1] if d == 0 else S.at[:, 0]
            found.append((d, None, None, plane, CXR.at[d, :, pl.ds(a_row, Y)], (to, at_a, gz)))
            found.append((2 + d, slide[d], recv_slide[d], plane, CXR.at[d, :, pl.ds(n_row, Y)], (to, at_n, gz)))
        return found

    def cyz_messages():
        found = [(4 + d, None, None, CYS.at[d], CYR.at[d], (gx, wrap(gy + 1 - 2 * d, ny), gz)) for d in range(2)]
        for step, slot in zs:
            found.append((6 + slot, None, None, CZS, CZR.at[slot], (gx, gy, wrap(gz + step, nz))))
        return found

    def when(predicate, action):
        if predicate is None:
            action()
        else:
            pl.when(predicate)(action)

    def copy_of(message, sems):
        index, _, _, source, destination, device = message
        return pltpu.make_async_remote_copy(
            src_ref=source, dst_ref=destination, send_sem=sems[0].at[index],
            recv_sem=sems[1].at[index], device_id=device, device_id_type=MESH)

    def send(messages, sems):
        for message in messages:
            when(message[1], lambda m=message: copy_of(m, sems).start())

    def await_received(messages, sems):
        for message in messages:
            when(message[2], lambda m=message: copy_of(m, sems).wait_recv())

    def await_sent(messages, sems):
        for message in messages:
            when(message[1], lambda m=message: copy_of(m, sems).wait_send())

    def field_sems(par):
        return send_sem, recv_sem.at[par]

    coef_sems = (csend_sem, crecv_sem)

    loads = [
        pltpu.make_async_copy(conc, F.at[pl.ds(2, X), pl.ds(8, Y)], load_sem.at[0]),
        pltpu.make_async_copy(diff, S.at[0], load_sem.at[1]),
        pltpu.make_async_copy(speed, SPD, load_sem.at[2]),
        pltpu.make_async_copy(signs, SGN, load_sem.at[3]),
    ]
    for load in loads:
        load.start()
    barrier = pltpu.get_barrier_semaphore()
    for message in x_messages(0) + yz_messages(0):
        when(message[1], lambda m=message: pl.semaphore_signal(
            barrier, inc=1, device_id=m[5], device_id_type=MESH))
    sliding = jnp.logical_or(slide[0], slide[1])

    @pl.when(sliding)
    def _():
        pl.semaphore_wait(barrier, 20)

    @pl.when(jnp.logical_not(sliding))
    def _():
        pl.semaphore_wait(barrier, 18)

    def roll(value, amount):
        amount = amount % Z
        return value if amount == 0 else pltpu.roll(value, amount, 1)

    def pack_xz():
        for d, p in ((0, X + 1), (1, 2)):
            packed = roll(F[p, pl.ds(8, 8)], 2)
            for yt in range(1, tiles):
                packed = jnp.where((lane >> 2) == yt, roll(F[p, pl.ds(8 + 8 * yt, 8)], 4 * yt + 2), packed)
            XZS[d] = packed

    def pack_z(get, put):
        def some(h, _):
            packed = roll(get(4 * h, 0), 2)
            for i in range(1, 32):
                packed = jnp.where((lane >> 2) == i, roll(get(4 * h + i // 8, i % 8), 4 * i + 2), packed)
            put(h, packed)
            return 0

        lax.fori_loop(0, 4, some, 0)

    def put_zs(h, value):
        ZS[h] = value

    def pack_yz():
        for d, near, far in ((0, 71, 70), (1, 8, 9)):
            YS[d, 0] = F[pl.ds(2, X), near, :]
            YS[d, 1] = F[pl.ds(2, X), far, :]
        pack_z(lambda p, yt: F[2 + p, pl.ds(8 + 8 * yt, 8)], put_zs)

    loads[0].wait()
    pack_xz()
    send(x_messages(0), field_sems(0))
    pack_yz()
    send(yz_messages(0), field_sems(0))

    for load in loads[1:]:
        load.wait()

    def own_coefficients(p):
        for yt in range(tiles):
            rows = pl.ds(8 * yt, 8)
            velocities = []
            for axis in range(3):
                magnitude = SPD[axis, p, rows]
                velocity = jnp.where(SGN[axis, p, rows] > 0, magnitude, -magnitude)
                S[1 + axis, p, rows] = velocity
                velocities.append(velocity)
            for k, weight in enumerate(coefficients(S[0, p, rows], velocities)):
                C[k, 1 + p, rows] = weight

    def outer_coefficients(i, _):
        own_coefficients((X - 1) * i)
        return 0

    def inner_coefficients(p, _):
        own_coefficients(p)
        return 0

    lax.fori_loop(0, 2, outer_coefficients, 0)
    send(cx_messages(), coef_sems)
    lax.fori_loop(1, X - 1, inner_coefficients, 0)
    for d, row in ((0, Y - 1), (1, 0)):
        for a in range(4):
            CYS[d, a] = S[a, :, row, :]
    for a in range(4):
        def put_czs(h, value, a=a):
            CZS[a, h] = value

        pack_z(lambda p, yt, a=a: S[a, p, pl.ds(8 * yt, 8)], put_czs)
    send(cyz_messages(), coef_sems)
    await_received(cyz_messages(), coef_sems)
    for d in range(2):
        values = [CYR[d, a] for a in range(4)]
        for k, weight in enumerate(coefficients(values[0], values[1:])):
            CY[d, k] = weight

    def ghost_coefficients(h, _):
        merged = [jnp.where(from_left, CZR[0, a, h], CZR[1, a, h]) for a in range(4)]
        for i in range(32):
            values = [roll(m, -(4 * i + 2)) for m in merged]
            for k, weight in enumerate(coefficients(values[0], values[1:])):
                CT[k, 4 * h + i // 8, pl.ds(8 * (i % 8), 8)] = weight
        return 0

    lax.fori_loop(0, 4, ghost_coefficients, 0)

    def along_z(value, other):
        return roll(jnp.where(l127, other, value), 1), roll(jnp.where(l0, other, value), -1)

    def tile_of(field, weights, p, yt, value, below, above):
        rows = pl.ds(8 + 8 * yt, 8)
        return weigh(weights, (
            value, field[p - 1, rows], field[p + 1, rows], field[p, pl.ds(7 + 8 * yt, 8)],
            field[p, pl.ds(9 + 8 * yt, 8)], below, above))

    def plane(source, ghost, target, p):
        for yt in range(tiles):
            rows = pl.ds(8 + 8 * yt, 8)
            value = source[p, rows]
            below, above = along_z(value, ghost[p, rows])
            weights = [C[k, p - 1, pl.ds(8 * yt, 8)] for k in range(7)]
            target[p, rows] = tile_of(source, weights, p, yt, value, below, above)

    def ghost_plane(p):
        for yt in range(tiles):
            rows = pl.ds(8 + 8 * yt, 8)
            value = T[p, rows]
            below, above = along_z(value, F[p, rows])
            weights = [CT[k, p - 2, pl.ds(8 * yt, 8)] for k in range(7)]
            T1[p, rows] = tile_of(T, weights, p, yt, value, below, above)

    def first_inner(p, _):
        plane(F, T, F1, p)
        ghost_plane(p)
        return 0

    def first_outer(i, _):
        p = 2 + (X - 1) * i
        plane(F, T, F1, p)
        ghost_plane(p)
        return 0

    def first_beyond(i, _):
        plane(F, T, F1, 1 + (X + 1) * i)
        return 0

    def second_inner(p, _):
        plane(F1, T1, F, p)
        return 0

    def second_outer(i, _):
        plane(F1, T1, F, jnp.where(i < 2, 2 + i, X - 2 + i))
        return 0

    def step_pair(m, _):
        par = lax.rem(m, 2)
        sems = field_sems(par)
        await_received(yz_messages(par), sems)

        def unpack(h, _):
            merged = jnp.where(from_left, ZR[par, 0, h], ZR[par, 1, h])
            for i in range(32):
                T[2 + 4 * h + i // 8, pl.ds(8 + 8 * (i % 8), 8)] = roll(merged, -(4 * i + 2))
            return 0

        lax.fori_loop(0, 4, unpack, 0)
        for d, row in ((0, 7), (1, 72)):
            F[pl.ds(2, X), row, :] = YR[par, d, 0]
            T[pl.ds(2, X), row, :] = jnp.where(low16, YZR[par, d, 1], YZR[par, d, 0])
        lax.fori_loop(3, X + 1, first_inner, 0)

        await_received(x_messages(par), sems)
        for d in range(2):
            a_row, n_row = (8, 72) if d == 0 else (72, 8)
            for block, row in ((0, a_row), (1, n_row)):
                merged = jnp.where(from_left, XZR[par, d, block, 0], XZR[par, d, block, 1])
                for yt in range(tiles):
                    ST[d, pl.ds(row + 8 * yt, 8)] = roll(merged, -(4 * yt + 2))
            for i in range(2):
                LB[d, i] = SB[par, d, i]
            for i in range(2):
                F[(X + 2) * d + i] = LB[d, i, pl.ds(start[d], 80)]
            T[1 + (X + 1) * d, pl.ds(8, Y)] = ST[d, pl.ds(start[d] + 8, Y)]

        @pl.when(m == 0)
        def _():
            await_received(cx_messages(), coef_sems)
            for d in range(2):
                for yt in range(tiles):
                    values = [CXR[d, a, pl.ds(start[d] + 8 + 8 * yt, 8)] for a in range(4)]
                    for k, weight in enumerate(coefficients(values[0], values[1:])):
                        C[k, (X + 1) * d, pl.ds(8 * yt, 8)] = weight

        lax.fori_loop(0, 2, first_beyond, 0)
        lax.fori_loop(0, 2, first_outer, 0)
        for d, row in ((0, 7), (1, 72)):
            value = YR[par, d, 0]
            below = roll(jnp.where(last16, YZR[par, d, 0], value), 1)
            above = roll(jnp.where(first16, YZR[par, d, 1], value), -1)
            far, own = YR[par, d, 1], F[pl.ds(2, X), 8 if d == 0 else 71, :]
            y_low, y_high = (far, own) if d == 0 else (own, far)
            F1[pl.ds(2, X), row, :] = weigh([CY[d, k] for k in range(7)], (
                value, F[pl.ds(1, X), row, :], F[pl.ds(3, X), row, :], y_low, y_high, below, above))
        await_sent(x_messages(par) + yz_messages(par), sems)

        lax.fori_loop(0, 4, second_outer, 0)

        @pl.when(m < rounds - 1)
        def _():
            pack_xz()
            send(x_messages(1 - par), field_sems(1 - par))

        lax.fori_loop(4, X, second_inner, 0)

        @pl.when(m < rounds - 1)
        def _():
            pack_yz()
            send(yz_messages(1 - par), field_sems(1 - par))

        return 0

    lax.fori_loop(0, rounds, step_pair, 0)
    await_sent(cx_messages() + cyz_messages(), coef_sems)
    result = pltpu.make_async_copy(F.at[pl.ds(2, X), pl.ds(8, Y)], out, out_sem)
    result.start()
    result.wait()


def body(sizes, concentration, speed, signs, diffusivity, shear):
    X, Y, Z = concentration.shape
    f32, vmem, dma = jnp.float32, pltpu.VMEM, pltpu.SemaphoreType.DMA
    hbm = pl.BlockSpec(memory_space=pl.ANY)

    def call(q, r, *arrays):
        return pl.pallas_call(
            functools.partial(kernel, q, sizes),
            out_shape=jax.ShapeDtypeStruct((X, Y, Z), f32),
            in_specs=[pl.BlockSpec(memory_space=pltpu.SMEM)] + [hbm] * 4,
            out_specs=hbm,
            scratch_shapes=[
                vmem((X + 4, Y + 16, Z), f32),
                vmem((X + 4, Y + 16, Z), f32),
                vmem((X + 4, Y + 16, Z), f32),
                vmem((X + 4, Y + 16, Z), f32),
                vmem((7, X + 2, Y, Z), f32),
                vmem((7, X, Y, Z), f32),
                vmem((2, 7, X, Z), f32),
                vmem((4, X, Y, Z), f32),
                vmem((3, X, Y, Z), f32),
                vmem((3, X, Y, Z), jnp.int32),
                vmem((2, 2, 2, 144, Z), f32),
                vmem((2, 2, 144, Z), f32),
                vmem((2, 144, Z), f32),
                vmem((2, 8, Z), f32),
                vmem((2, 2, 2, 2, 8, Z), f32),
                vmem((2, 2, X, Z), f32),
                vmem((2, 2, 2, X, Z), f32),
                vmem((2, 2, 2, X, Z), f32),
                vmem((4, 8, Z), f32),
                vmem((2, 2, 4, 8, Z), f32),
                vmem((2, 4, 144, Z), f32),
                vmem((2, 4, X, Z), f32),
                vmem((2, 4, X, Z), f32),
                vmem((4, 4, 8, Z), f32),
                vmem((2, 4, 4, 8, Z), f32),
                dma((4,)), dma((22,)), dma((2, 22)), dma((8,)), dma((8,)), dma(()),
            ],
            compiler_params=pltpu.CompilerParams(
                collective_id=q, has_side_effects=True, vmem_limit_bytes=48 << 20),
        )(r, *arrays)

    offset = lax.rem(shear[0], sizes[1] * Y)
    branches = [functools.partial(call, q) for q in range(sizes[1])]
    return lax.switch(offset // Y, branches, (offset % Y)[None], concentration, speed, signs, diffusivity)


def solution(mesh):
    sizes = tuple(mesh.shape[name] for name in ("gx", "gy", "gz"))
    placed = (
        P("gx", "gy", "gz"),
        P(None, "gx", "gy", "gz"),
        P(None, "gx", "gy", "gz"),
        P("gx", "gy", "gz"),
        P(),
    )
    return jax.shard_map(
        functools.partial(body, sizes), mesh=mesh, in_specs=placed, out_specs=P("gx", "gy", "gz"), check_vma=False
    )
```

```python
import functools

import jax
import jax.numpy as jnp
from jax import lax
from jax.experimental import pallas as pl
from jax.experimental.pallas import tpu as pltpu
from jax.sharding import PartitionSpec as P

STEPS = 8
DT = 0.25
MESH = pl.DeviceIdType.MESH


def coefficients(diffusivity, velocities):
    base = DT * diffusivity
    sides = []
    for velocity in velocities:
        sides.append(base + DT * jnp.maximum(velocity, 0.0))
        sides.append(base + DT * jnp.minimum(velocity, 0.0))
    own = 1.0
    for side in sides:
        own = own - side
    return [own] + sides


def weigh(weights, cells):
    total = weights[0] * cells[0]
    for weight, cell in zip(weights[1:], cells[1:]):
        total = total + weight * cell
    return total


def kernel(q, sizes, r_ref, conc, speed, signs, diff, out, F, T, F1, T1, C, CT, CY, S, SPD, SGN, SB, LB, ST, XZS, XZR,
           YS, YR, YZR, ZS, ZR, CXR, CYS, CYR, CZS, CZR, load_sem, send_sem, recv_sem, csend_sem, crecv_sem, out_sem):
    nx, ny, nz = sizes
    X, Y, Z = 16, 64, 128
    tiles = Y // 8
    rounds = STEPS // 2
    gx, gy, gz = lax.axis_index("gx"), lax.axis_index("gy"), lax.axis_index("gz")
    lane = lax.broadcasted_iota(jnp.int32, (8, Z), 1)
    l0, l127, from_left = lane == 0, lane == Z - 1, (lane & 2) == 0
    lane16 = lax.broadcasted_iota(jnp.int32, (X, Z), 1)
    first16, last16, low16 = lane16 == 0, lane16 == Z - 1, lane16 < 64
    r = r_ref[0]
    slide = (gx == nx - 1, gx == 0)
    recv_slide = (gx == 0, gx == nx - 1)
    start = (jnp.where(recv_slide[0], r, 0), jnp.where(recv_slide[1], 64 - r, 64))

    def wrap(value, n):
        return lax.rem(value + 2 * n, n)

    def x_targets(d):
        sign = 1 if d == 0 else -1
        to = wrap(gx + sign, nx)
        shift = jnp.where(slide[d], q, 0) * sign
        return to, wrap(gy - shift, ny), wrap(gy - shift - sign, ny), wrap(gy - shift + sign, ny)

    zs = ((1, 0), (-1, 1))

    def x_messages(par):
        found = []
        for d in range(2):
            to, at_a, at_n, at_e = x_targets(d)
            yes, no = slide[d], jnp.logical_not(slide[d])
            ryes, rno = recv_slide[d], jnp.logical_not(recv_slide[d])
            planes = F.at[pl.ds(X, 2), pl.ds(8, Y)] if d == 0 else F.at[pl.ds(2, 2), pl.ds(8, Y)]
            near, near_slot = (X + 1, 1) if d == 0 else (2, 0)
            first, last = F.at[near, pl.ds(8, 8)], F.at[near, pl.ds(Y, 8)]
            a_row, n_row = (8, 72) if d == 0 else (72, 8)
            found.append((d, None, None, planes, SB.at[par, d, :, pl.ds(a_row, Y)], (to, at_a, gz)))
            found.append((2 + d, yes, ryes, planes, SB.at[par, d, :, pl.ds(n_row, Y)], (to, at_n, gz)))
            if d == 0:
                found.append((2 + d, no, rno, first, SB.at[par, d, near_slot, pl.ds(72, 8)], (to, at_n, gz)))
                found.append((4 + d, None, None, last, SB.at[par, d, near_slot, pl.ds(0, 8)], (to, at_e, gz)))
            else:
                found.append((2 + d, no, rno, last, SB.at[par, d, near_slot, pl.ds(64, 8)], (to, at_n, gz)))
                found.append((4 + d, None, None, first, SB.at[par, d, near_slot, pl.ds(136, 8)], (to, at_e, gz)))
            for step, slot in zs:
                side = wrap(gz + step, nz)
                found.append((6 + 2 * d + slot, None, None, XZS.at[d], XZR.at[par, d, 0, slot], (to, at_a, side)))
                found.append((10 + 2 * d + slot, yes, ryes, XZS.at[d], XZR.at[par, d, 1, slot], (to, at_n, side)))
        return found

    def yz_messages(par):
        found = []
        for d in range(2):
            to = wrap(gy + 1 - 2 * d, ny)
            found.append((14 + d, None, None, YS.at[d], YR.at[par, d], (gx, to, gz)))
            for step, slot in zs:
                found.append((18 + 2 * d + slot, None, None, YS.at[d, 0], YZR.at[par, d, slot],
                              (gx, to, wrap(gz + step, nz))))
        for step, slot in zs:
            found.append((16 + slot, None, None, ZS, ZR.at[par, slot], (gx, gy, wrap(gz + step, nz))))
        return found

    def cx_messages():
        found = []
        for d in range(2):
            to, at_a, _, _ = x_targets(d)
            plane = S.at[:, pl.ds(Y * (X - 1), Y)] if d == 0 else S.at[:, pl.ds(0, Y)]
            found.append((d, None, None, plane, CXR.at[d, :, pl.ds(8 if d == 0 else 72, Y)], (to, at_a, gz)))
        return found

    def cx_forwards():
        found = []
        for d in range(2):
            a_row, n_row = (8, 72) if d == 0 else (72, 8)
            found.append((2 + d, recv_slide[d], recv_slide[d], CXR.at[d, :, pl.ds(a_row, Y)],
                          CXR.at[d, :, pl.ds(n_row, Y)], (gx, wrap(gy - 1 + 2 * d, ny), gz)))
        return found

    def cyz_messages():
        found = [(4 + d, None, None, CYS.at[d], CYR.at[d], (gx, wrap(gy + 1 - 2 * d, ny), gz)) for d in range(2)]
        for step, slot in zs:
            found.append((6 + slot, None, None, CZS, CZR.at[slot], (gx, gy, wrap(gz + step, nz))))
        return found

    def when(predicate, action):
        if predicate is None:
            action()
        else:
            pl.when(predicate)(action)

    def copy_of(message, sems):
        index, _, _, source, destination, device = message
        return pltpu.make_async_remote_copy(
            src_ref=source, dst_ref=destination, send_sem=sems[0].at[index],
            recv_sem=sems[1].at[index], device_id=device, device_id_type=MESH)

    def send(messages, sems):
        for message in messages:
            when(message[1], lambda m=message: copy_of(m, sems).start())

    def await_received(messages, sems):
        for message in messages:
            when(message[2], lambda m=message: copy_of(m, sems).wait_recv())

    def await_sent(messages, sems):
        for message in messages:
            when(message[1], lambda m=message: copy_of(m, sems).wait_send())

    def field_sems(par):
        return send_sem, recv_sem.at[par]

    coef_sems = (csend_sem, crecv_sem)

    loads = [
        pltpu.make_async_copy(conc, F.at[pl.ds(2, X), pl.ds(8, Y)], load_sem.at[0]),
        pltpu.make_async_copy(diff, S.at[0, pl.ds(0, X * Y)], load_sem.at[1]),
        pltpu.make_async_copy(speed, SPD.at[:, pl.ds(0, X * Y)], load_sem.at[2]),
        pltpu.make_async_copy(signs, SGN.at[:, pl.ds(0, X * Y)], load_sem.at[3]),
    ]
    for load in loads:
        load.start()
    barrier = pltpu.get_barrier_semaphore()
    for message in x_messages(0) + yz_messages(0):
        when(message[1], lambda m=message: pl.semaphore_signal(
            barrier, inc=1, device_id=m[5], device_id_type=MESH))

    def roll(value, amount):
        amount = amount % Z
        return value if amount == 0 else pltpu.roll(value, amount, 1)

    def pack_xz():
        for d, p in ((0, X + 1), (1, 2)):
            packed = roll(F[p, pl.ds(8, 8)], 2)
            for yt in range(1, tiles):
                packed = jnp.where((lane >> 2) == yt, roll(F[p, pl.ds(8 + 8 * yt, 8)], 4 * yt + 2), packed)
            XZS[d] = packed

    def pack_z(get, put):
        def some(h, _):
            packed = roll(get(4 * h, 0), 2)
            for i in range(1, 32):
                packed = jnp.where((lane >> 2) == i, roll(get(4 * h + i // 8, i % 8), 4 * i + 2), packed)
            put(h, packed)
            return 0

        for h in range(4):
            some(h, 0)

    def put_zs(h, value):
        ZS[h] = value

    def pack_yz():
        for d, near, far in ((0, 71, 70), (1, 8, 9)):
            YS[d, 0] = F[pl.ds(2, X), near, :]
            YS[d, 1] = F[pl.ds(2, X), far, :]
        pack_z(lambda p, yt: F[2 + p, pl.ds(8 + 8 * yt, 8)], put_zs)

    loads[0].wait()
    pack_xz()
    pack_yz()
    for load in loads[1:]:
        load.wait()

    def own_coefficients(p):
        for yt in range(tiles):
            rows = pl.ds(pl.multiple_of(Y * p + 8 * yt, 8), 8)
            velocities = []
            for axis in range(3):
                magnitude = SPD[axis, rows]
                velocity = jnp.where(SGN[axis, rows] > 0, magnitude, -magnitude)
                S[1 + axis, rows] = velocity
                velocities.append(velocity)
            for k, weight in enumerate(coefficients(S[0, rows], velocities)):
                C[tiles * (1 + p) + yt, k] = weight

    def each_coefficients(p, _):
        own_coefficients(p)
        return 0

    lax.fori_loop(0, X, each_coefficients, 0)
    for d, row in ((0, Y - 1), (1, 0)):
        for a in range(4):
            CYS[d, a] = S[a, pl.ds(row, X, stride=Y), :]
    def pack_coefficients(a, _):
        def put_czs(h, value):
            CZS[a, h] = value

        pack_z(lambda p, yt: S[a, pl.ds(Y * p + 8 * yt, 8)], put_czs)
        return 0

    lax.fori_loop(0, 4, pack_coefficients, 0)
    sliding = jnp.logical_or(slide[0], slide[1])

    @pl.when(sliding)
    def _():
        pl.semaphore_wait(barrier, 20)

    @pl.when(jnp.logical_not(sliding))
    def _():
        pl.semaphore_wait(barrier, 18)

    send(x_messages(0), field_sems(0))
    send(yz_messages(0), field_sems(0))
    send(cyz_messages(), coef_sems)
    send(cx_messages(), coef_sems)
    await_received(cyz_messages(), coef_sems)
    for d in range(2):
        values = [CYR[d, a] for a in range(4)]
        for k, weight in enumerate(coefficients(values[0], values[1:])):
            CY[d, k] = weight

    def ghost_coefficients(h, _):
        merged = [jnp.where(from_left, CZR[0, a, h], CZR[1, a, h]) for a in range(4)]
        for i in range(32):
            values = [roll(m, -(4 * i + 2)) for m in merged]
            for k, weight in enumerate(coefficients(values[0], values[1:])):
                CT[32 * h + i, k] = weight
        return 0

    lax.fori_loop(0, 4, ghost_coefficients, 0)

    def along_z(value, other):
        return roll(jnp.where(l127, other, value), 1), roll(jnp.where(l0, other, value), -1)

    def tile_of(field, weights, p, yt, value, below, above):
        rows = pl.ds(8 + 8 * yt, 8)
        return weigh(weights, (
            value, field[p - 1, rows], field[p + 1, rows], field[p, pl.ds(7 + 8 * yt, 8)],
            field[p, pl.ds(9 + 8 * yt, 8)], below, above))

    def plane(source, ghost, target, p):
        for yt in range(tiles):
            rows = pl.ds(8 + 8 * yt, 8)
            value = source[p, rows]
            below, above = along_z(value, ghost[p, rows])
            weights = [C[tiles * (p - 1) + yt, k] for k in range(7)]
            target[p, rows] = tile_of(source, weights, p, yt, value, below, above)

    def ghost_plane(p):
        for yt in range(tiles):
            rows = pl.ds(8 + 8 * yt, 8)
            value = T[p, rows]
            below, above = along_z(value, F[p, rows])
            weights = [CT[tiles * (p - 2) + yt, k] for k in range(7)]
            T1[p, rows] = tile_of(T, weights, p, yt, value, below, above)

    def first_inner(i, _):
        for p in (3 + 2 * i, 4 + 2 * i):
            plane(F, T, F1, p)
            ghost_plane(p)
        return 0

    def second_inner(i, _):
        for p in range(4):
            plane(F1, T1, F, 4 + 4 * i + p)
        return 0

    def step_pair(m, _):
        par = lax.rem(m, 2)
        sems = field_sems(par)
        await_received(yz_messages(par), sems)

        def unpack(h, _):
            merged = jnp.where(from_left, ZR[par, 0, h], ZR[par, 1, h])
            for i in range(32):
                T[2 + 4 * h + i // 8, pl.ds(8 + 8 * (i % 8), 8)] = roll(merged, -(4 * i + 2))
            return 0

        for h in range(4):
            unpack(h, 0)
        for d, row in ((0, 7), (1, 72)):
            F[pl.ds(2, X), row, :] = YR[par, d, 0]
            T[pl.ds(2, X), row, :] = jnp.where(low16, YZR[par, d, 1], YZR[par, d, 0])
        lax.fori_loop(0, X // 2 - 1, first_inner, 0)

        @pl.when(m == 0)
        def _():
            await_received(cx_messages(), coef_sems)
            send(cx_forwards(), coef_sems)

        await_received(x_messages(par), sems)
        for d in range(2):
            a_row, n_row = (8, 72) if d == 0 else (72, 8)
            for block, row in ((0, a_row), (1, n_row)):
                merged = jnp.where(from_left, XZR[par, d, block, 0], XZR[par, d, block, 1])
                for yt in range(tiles):
                    ST[d, pl.ds(row + 8 * yt, 8)] = roll(merged, -(4 * yt + 2))
            for i in range(2):
                LB[d, i] = SB[par, d, i]
            for i in range(2):
                F[(X + 2) * d + i, pl.ds(0, 80)] = LB[d, i, pl.ds(start[d], 80)]
            T[1 + (X + 1) * d, pl.ds(8, Y)] = ST[d, pl.ds(start[d] + 8, Y)]

        @pl.when(m == 0)
        def _():
            await_received(cx_forwards(), coef_sems)
            for d in range(2):
                for yt in range(tiles):
                    values = [CXR[d, a, pl.ds(start[d] + 8 + 8 * yt, 8)] for a in range(4)]
                    for k, weight in enumerate(coefficients(values[0], values[1:])):
                        C[tiles * (X + 1) * d + yt, k] = weight

        for p in (1, X + 2, 2, X + 1):
            plane(F, T, F1, p)
        for p in (2, X + 1):
            ghost_plane(p)
        for d, row in ((0, 7), (1, 72)):
            value = YR[par, d, 0]
            below = roll(jnp.where(last16, YZR[par, d, 0], value), 1)
            above = roll(jnp.where(first16, YZR[par, d, 1], value), -1)
            far, own = YR[par, d, 1], F[pl.ds(2, X), 8 if d == 0 else 71, :]
            y_low, y_high = (far, own) if d == 0 else (own, far)
            F1[pl.ds(2, X), row, :] = weigh([CY[d, k] for k in range(7)], (
                value, F[pl.ds(1, X), row, :], F[pl.ds(3, X), row, :], y_low, y_high, below, above))
        await_sent(x_messages(par) + yz_messages(par), sems)

        for p in (2, 3, X, X + 1):
            plane(F1, T1, F, p)

        @pl.when(m < rounds - 1)
        def _():
            pack_xz()
            send(x_messages(1 - par), field_sems(1 - par))

        lax.fori_loop(0, X // 4 - 1, second_inner, 0)

        @pl.when(m < rounds - 1)
        def _():
            pack_yz()
            send(yz_messages(1 - par), field_sems(1 - par))

        return 0

    lax.fori_loop(0, rounds, step_pair, 0)
    await_sent(cx_messages() + cx_forwards() + cyz_messages(), coef_sems)
    result = pltpu.make_async_copy(F.at[pl.ds(2, X), pl.ds(8, Y)], out, out_sem)
    result.start()
    result.wait()


def body(sizes, concentration, speed, signs, diffusivity, shear):
    X, Y, Z = concentration.shape
    f32, vmem, dma = jnp.float32, pltpu.VMEM, pltpu.SemaphoreType.DMA
    hbm = pl.BlockSpec(memory_space=pl.ANY)

    def call(q, r, *arrays):
        return pl.pallas_call(
            functools.partial(kernel, q, sizes),
            out_shape=jax.ShapeDtypeStruct((X, Y, Z), f32),
            in_specs=[pl.BlockSpec(memory_space=pltpu.SMEM)] + [hbm] * 4,
            out_specs=hbm,
            scratch_shapes=[
                vmem((X + 4, Y + 24, Z), f32),
                vmem((X + 4, Y + 24, Z), f32),
                vmem((X + 4, Y + 24, Z), f32),
                vmem((X + 4, Y + 24, Z), f32),
                vmem(((X + 2) * Y // 8, 7, 8, Z), f32),
                vmem((X * Y // 8, 7, 8, Z), f32),
                vmem((2, 7, X, Z), f32),
                vmem((4, X * Y + 8, Z), f32),
                vmem((3, X * Y + 8, Z), f32),
                vmem((3, X * Y + 8, Z), jnp.int32),
                vmem((2, 2, 2, 144, Z), f32),
                vmem((2, 2, 144, Z), f32),
                vmem((2, 144, Z), f32),
                vmem((2, 8, Z), f32),
                vmem((2, 2, 2, 2, 8, Z), f32),
                vmem((2, 2, X, Z), f32),
                vmem((2, 2, 2, X, Z), f32),
                vmem((2, 2, 2, X, Z), f32),
                vmem((4, 8, Z), f32),
                vmem((2, 2, 4, 8, Z), f32),
                vmem((2, 4, 144, Z), f32),
                vmem((2, 4, X, Z), f32),
                vmem((2, 4, X, Z), f32),
                vmem((4, 4, 8, Z), f32),
                vmem((2, 4, 4, 8, Z), f32),
                dma((4,)), dma((22,)), dma((2, 22)), dma((8,)), dma((8,)), dma(()),
            ],
            compiler_params=pltpu.CompilerParams(
                collective_id=q, has_side_effects=True, vmem_limit_bytes=48 << 20),
        )(r, *arrays)

    offset = lax.rem(shear[0], sizes[1] * Y)
    branches = [functools.partial(call, q) for q in range(sizes[1])]
    return lax.switch(offset // Y, branches, (offset % Y)[None], concentration,
                      speed.reshape(3, X * Y, Z), signs.reshape(3, X * Y, Z), diffusivity.reshape(X * Y, Z))


def solution(mesh):
    sizes = tuple(mesh.shape[name] for name in ("gx", "gy", "gz"))
    placed = (
        P("gx", "gy", "gz"),
        P(None, "gx", "gy", "gz"),
        P(None, "gx", "gy", "gz"),
        P("gx", "gy", "gz"),
        P(),
    )
    return jax.shard_map(
        functools.partial(body, sizes), mesh=mesh, in_specs=placed, out_specs=P("gx", "gy", "gz"), check_vma=False
    )
```

```python
import functools

import jax
import jax.numpy as jnp
from jax import lax
from jax.experimental import pallas as pl
from jax.experimental.pallas import tpu as pltpu
from jax.sharding import PartitionSpec as P

STEPS = 8
DT = 0.25
MESH = pl.DeviceIdType.MESH


def coefficients(diffusivity, velocities):
    base = DT * diffusivity
    sides = []
    for velocity in velocities:
        sides.append(base + DT * jnp.maximum(velocity, 0.0))
        sides.append(base + DT * jnp.minimum(velocity, 0.0))
    own = 1.0
    for side in sides:
        own = own - side
    return [own] + sides


def weigh(weights, cells):
    total = weights[0] * cells[0]
    for weight, cell in zip(weights[1:], cells[1:]):
        total = total + weight * cell
    return total


def kernel(q, sizes, r_ref, conc, speed, signs, diff, out, F, T, F1, T1, C, CT, CY, S, SPD, SGN, SB, LB, ST, XZS, XZR,
           YS, YR, YZR, ZS, ZR, CXR, CYS, CYR, CZS, CZR, load_sem, send_sem, recv_sem, csend_sem, crecv_sem, out_sem):
    nx, ny, nz = sizes
    X, Y, Z = 16, 64, 128
    tiles = Y // 8
    rounds = STEPS // 2
    gx, gy, gz = lax.axis_index("gx"), lax.axis_index("gy"), lax.axis_index("gz")
    lane = lax.broadcasted_iota(jnp.int32, (8, Z), 1)
    l0, l127, from_left = lane == 0, lane == Z - 1, (lane & 2) == 0
    lane16 = lax.broadcasted_iota(jnp.int32, (X, Z), 1)
    first16, last16, low16 = lane16 == 0, lane16 == Z - 1, lane16 < 64
    r = r_ref[0]
    slide = (gx == nx - 1, gx == 0)
    recv_slide = (gx == 0, gx == nx - 1)
    start = (jnp.where(recv_slide[0], r, 0), jnp.where(recv_slide[1], 64 - r, 64))

    def wrap(value, n):
        return lax.rem(value + 2 * n, n)

    def x_targets(d):
        sign = 1 if d == 0 else -1
        to = wrap(gx + sign, nx)
        shift = jnp.where(slide[d], q, 0) * sign
        return to, wrap(gy - shift, ny), wrap(gy - shift - sign, ny), wrap(gy - shift + sign, ny)

    zs = ((1, 0), (-1, 1))

    def x_messages(par):
        found, no_slide = [], []
        for d in range(2):
            to, at_a, at_n, at_e = x_targets(d)
            yes, no = slide[d], jnp.logical_not(slide[d])
            ryes, rno = recv_slide[d], jnp.logical_not(recv_slide[d])
            no_slide.append(no)
            planes = F.at[pl.ds(X, 2), pl.ds(8, Y)] if d == 0 else F.at[pl.ds(2, 2), pl.ds(8, Y)]
            near, near_slot = (X + 1, 1) if d == 0 else (2, 0)
            first, last = F.at[near, pl.ds(8, 8)], F.at[near, pl.ds(Y, 8)]
            a_row, n_row = (8, 72) if d == 0 else (72, 8)
            found.append((d, None, None, planes, SB.at[par, d, :, pl.ds(a_row, Y)], (to, at_a, gz)))
            found.append((2 + d, yes, ryes, planes, SB.at[par, d, :, pl.ds(n_row, Y)], (to, at_n, gz)))
            if d == 0:
                found.append((2 + d, no, rno, first, SB.at[par, d, near_slot, pl.ds(72, 8)], (to, at_n, gz)))
                found.append((4 + d, None, None, last, SB.at[par, d, near_slot, pl.ds(0, 8)], (to, at_e, gz)))
            else:
                found.append((2 + d, no, rno, last, SB.at[par, d, near_slot, pl.ds(64, 8)], (to, at_n, gz)))
                found.append((4 + d, None, None, first, SB.at[par, d, near_slot, pl.ds(136, 8)], (to, at_e, gz)))
            for step, slot in zs:
                side = wrap(gz + step, nz)
                found.append((6 + 2 * d + slot, None, None, XZS.at[d], XZR.at[par, d, 0, slot], (to, at_a, side)))
                found.append((10 + 2 * d + slot, yes, ryes, XZS.at[d], XZR.at[par, d, 1, slot], (to, at_n, side)))
        return sorted(found, key=lambda message: (message[0] < 4 and message[1] is not no_slide[message[0] % 2], message[0] // 2 == 1, -message[0]))

    def yz_messages(par):
        found = []
        for d in range(2):
            to = wrap(gy + 1 - 2 * d, ny)
            found.append((14 + d, None, None, YS.at[d], YR.at[par, d], (gx, to, gz)))
            for step, slot in zs:
                found.append((18 + 2 * d + slot, None, None, YS.at[d, 0], YZR.at[par, d, slot],
                              (gx, to, wrap(gz + step, nz))))
        for step, slot in zs:
            found.append((16 + slot, None, None, ZS, ZR.at[par, slot], (gx, gy, wrap(gz + step, nz))))
        return sorted(found, key=lambda message: -message[0])

    def cx_messages():
        found = []
        for d in range(2):
            to, at_a, _, _ = x_targets(d)
            plane = S.at[:, pl.ds(Y * (X - 1), Y)] if d == 0 else S.at[:, pl.ds(0, Y)]
            found.append((d, None, None, plane, CXR.at[d, :, pl.ds(8 if d == 0 else 72, Y)], (to, at_a, gz)))
        return found

    def cx_forwards():
        found = []
        for d in range(2):
            a_row, n_row = (8, 72) if d == 0 else (72, 8)
            found.append((2 + d, recv_slide[d], recv_slide[d], CXR.at[d, :, pl.ds(a_row, Y)],
                          CXR.at[d, :, pl.ds(n_row, Y)], (gx, wrap(gy - 1 + 2 * d, ny), gz)))
        return found

    def cyz_messages():
        found = [(4 + d, None, None, CYS.at[d], CYR.at[d], (gx, wrap(gy + 1 - 2 * d, ny), gz)) for d in range(2)]
        for step, slot in zs:
            found.append((6 + slot, None, None, CZS, CZR.at[slot], (gx, gy, wrap(gz + step, nz))))
        return found

    def when(predicate, action):
        if predicate is None:
            action()
        else:
            pl.when(predicate)(action)

    def copy_of(message, sems):
        index, _, _, source, destination, device = message
        return pltpu.make_async_remote_copy(
            src_ref=source, dst_ref=destination, send_sem=sems[0].at[index],
            recv_sem=sems[1].at[index], device_id=device, device_id_type=MESH)

    def send(messages, sems):
        for message in messages:
            when(message[1], lambda m=message: copy_of(m, sems).start())

    def await_received(messages, sems):
        for message in messages:
            when(message[2], lambda m=message: copy_of(m, sems).wait_recv())

    def await_sent(messages, sems):
        for message in messages:
            when(message[1], lambda m=message: copy_of(m, sems).wait_send())

    def field_sems(par):
        return send_sem, recv_sem.at[par]

    coef_sems = (csend_sem, crecv_sem)

    loads = [
        pltpu.make_async_copy(conc, F.at[pl.ds(2, X), pl.ds(8, Y)], load_sem.at[0]),
        pltpu.make_async_copy(diff, S.at[0, pl.ds(0, X * Y)], load_sem.at[1]),
        pltpu.make_async_copy(speed, SPD.at[:, pl.ds(0, X * Y)], load_sem.at[2]),
        pltpu.make_async_copy(signs, SGN.at[:, pl.ds(0, X * Y)], load_sem.at[3]),
    ]
    for load in loads:
        load.start()
    barrier = pltpu.get_barrier_semaphore()
    for message in x_messages(0) + yz_messages(0):
        when(message[1], lambda m=message: pl.semaphore_signal(
            barrier, inc=1, device_id=m[5], device_id_type=MESH))

    def roll(value, amount):
        amount = amount % Z
        return value if amount == 0 else pltpu.roll(value, amount, 1)

    def pack_xz():
        for d, p in ((0, X + 1), (1, 2)):
            packed = roll(F[p, pl.ds(8, 8)], 2)
            for yt in range(1, tiles):
                packed = jnp.where((lane >> 2) == yt, roll(F[p, pl.ds(8 + 8 * yt, 8)], 4 * yt + 2), packed)
            XZS[d] = packed

    def pack_z(get, put):
        def some(h, _):
            packed = roll(get(4 * h, 0), 2)
            for i in range(1, 32):
                packed = jnp.where((lane >> 2) == i, roll(get(4 * h + i // 8, i % 8), 4 * i + 2), packed)
            put(h, packed)
            return 0

        for h in range(4):
            some(h, 0)

    def put_zs(h, value):
        ZS[h] = value

    def pack_yz():
        for d, near, far in ((0, 71, 70), (1, 8, 9)):
            YS[d, 0] = F[pl.ds(2, X), near, :]
            YS[d, 1] = F[pl.ds(2, X), far, :]
        pack_z(lambda p, yt: F[2 + p, pl.ds(8 + 8 * yt, 8)], put_zs)

    loads[0].wait()
    pack_xz()
    sliding = jnp.logical_or(slide[0], slide[1])

    @pl.when(sliding)
    def _():
        pl.semaphore_wait(barrier, 20)

    @pl.when(jnp.logical_not(sliding))
    def _():
        pl.semaphore_wait(barrier, 18)

    send(x_messages(0), field_sems(0))
    pack_yz()
    send(yz_messages(0), field_sems(0))
    for load in loads[1:]:
        load.wait()

    def own_coefficients(p):
        for yt in range(tiles):
            rows = pl.ds(Y * p + 8 * yt, 8) if isinstance(p, int) else pl.ds(pl.multiple_of(Y * p + 8 * yt, 8), 8)
            velocities = []
            for axis in range(3):
                magnitude = SPD[axis, rows]
                velocity = jnp.where(SGN[axis, rows] > 0, magnitude, -magnitude)
                S[1 + axis, rows] = velocity
                velocities.append(velocity)
            for k, weight in enumerate(coefficients(S[0, rows], velocities)):
                C[tiles * (1 + p) + yt, k] = weight

    def each_coefficients(p, _):
        own_coefficients(p)
        return 0

    own_coefficients(0)
    own_coefficients(X - 1)
    send(cx_messages(), coef_sems)
    lax.fori_loop(1, X - 1, each_coefficients, 0)
    for d, row in ((0, Y - 1), (1, 0)):
        for a in range(4):
            CYS[d, a] = S[a, pl.ds(row, X, stride=Y), :]
    def pack_coefficients(a, _):
        def put_czs(h, value):
            CZS[a, h] = value

        pack_z(lambda p, yt: S[a, pl.ds(Y * p + 8 * yt, 8)], put_czs)
        return 0

    lax.fori_loop(0, 4, pack_coefficients, 0)
    send(cyz_messages(), coef_sems)
    await_received(cyz_messages(), coef_sems)
    for d in range(2):
        values = [CYR[d, a] for a in range(4)]
        for k, weight in enumerate(coefficients(values[0], values[1:])):
            CY[d, k] = weight

    def ghost_coefficients(h, _):
        merged = [jnp.where(from_left, CZR[0, a, h], CZR[1, a, h]) for a in range(4)]
        for i in range(32):
            values = [roll(m, -(4 * i + 2)) for m in merged]
            for k, weight in enumerate(coefficients(values[0], values[1:])):
                CT[32 * h + i, k] = weight
        return 0

    lax.fori_loop(0, 4, ghost_coefficients, 0)

    def along_z(value, other):
        return roll(jnp.where(l127, other, value), 1), roll(jnp.where(l0, other, value), -1)

    def tile_of(field, weights, p, yt, value, below, above):
        rows = pl.ds(8 + 8 * yt, 8)
        return weigh(weights, (
            value, field[p - 1, rows], field[p + 1, rows], field[p, pl.ds(7 + 8 * yt, 8)],
            field[p, pl.ds(9 + 8 * yt, 8)], below, above))

    def plane(source, ghost, target, p):
        for yt in range(tiles):
            rows = pl.ds(8 + 8 * yt, 8)
            value = source[p, rows]
            below, above = along_z(value, ghost[p, rows])
            weights = [C[tiles * (p - 1) + yt, k] for k in range(7)]
            target[p, rows] = tile_of(source, weights, p, yt, value, below, above)

    def ghost_plane(p):
        for yt in range(tiles):
            rows = pl.ds(8 + 8 * yt, 8)
            value = T[p, rows]
            below, above = along_z(value, F[p, rows])
            weights = [CT[tiles * (p - 2) + yt, k] for k in range(7)]
            T1[p, rows] = tile_of(T, weights, p, yt, value, below, above)

    def first_inner(i, _):
        for p in (3 + 2 * i, 4 + 2 * i):
            plane(F, T, F1, p)
            ghost_plane(p)
        return 0

    def second_inner(i, _):
        for p in range(4):
            plane(F1, T1, F, 4 + 4 * i + p)
        return 0

    def step_pair(m, _):
        par = lax.rem(m, 2)
        sems = field_sems(par)
        await_received(yz_messages(par), sems)

        def unpack(h, _):
            merged = jnp.where(from_left, ZR[par, 0, h], ZR[par, 1, h])
            for i in range(32):
                T[2 + 4 * h + i // 8, pl.ds(8 + 8 * (i % 8), 8)] = roll(merged, -(4 * i + 2))
            return 0

        for h in range(4):
            unpack(h, 0)
        for d, row in ((0, 7), (1, 72)):
            F[pl.ds(2, X), row, :] = YR[par, d, 0]
            T[pl.ds(2, X), row, :] = jnp.where(low16, YZR[par, d, 1], YZR[par, d, 0])
        lax.fori_loop(0, X // 2 - 1, first_inner, 0)

        @pl.when(m == 0)
        def _():
            await_received(cx_messages(), coef_sems)
            send(cx_forwards(), coef_sems)

        await_received(x_messages(par), sems)
        for d in range(2):
            a_row, n_row = (8, 72) if d == 0 else (72, 8)
            for block, row in ((0, a_row), (1, n_row)):
                merged = jnp.where(from_left, XZR[par, d, block, 0], XZR[par, d, block, 1])
                for yt in range(tiles):
                    ST[d, pl.ds(row + 8 * yt, 8)] = roll(merged, -(4 * yt + 2))
            for i in range(2):
                LB[d, i] = SB[par, d, i]
            for i in range(2):
                F[(X + 2) * d + i, pl.ds(0, 80)] = LB[d, i, pl.ds(start[d], 80)]
            T[1 + (X + 1) * d, pl.ds(8, Y)] = ST[d, pl.ds(start[d] + 8, Y)]

        @pl.when(m == 0)
        def _():
            await_received(cx_forwards(), coef_sems)
            for d in range(2):
                for yt in range(tiles):
                    values = [CXR[d, a, pl.ds(start[d] + 8 + 8 * yt, 8)] for a in range(4)]
                    for k, weight in enumerate(coefficients(values[0], values[1:])):
                        C[tiles * (X + 1) * d + yt, k] = weight

        for p in (1, X + 2, 2, X + 1):
            plane(F, T, F1, p)
        for p in (2, X + 1):
            ghost_plane(p)
        for d, row in ((0, 7), (1, 72)):
            value = YR[par, d, 0]
            below = roll(jnp.where(last16, YZR[par, d, 0], value), 1)
            above = roll(jnp.where(first16, YZR[par, d, 1], value), -1)
            far, own = YR[par, d, 1], F[pl.ds(2, X), 8 if d == 0 else 71, :]
            y_low, y_high = (far, own) if d == 0 else (own, far)
            F1[pl.ds(2, X), row, :] = weigh([CY[d, k] for k in range(7)], (
                value, F[pl.ds(1, X), row, :], F[pl.ds(3, X), row, :], y_low, y_high, below, above))
        await_sent(x_messages(par) + yz_messages(par), sems)

        for p in (2, 3, X, X + 1):
            plane(F1, T1, F, p)

        @pl.when(m < rounds - 1)
        def _():
            pack_xz()
            send(x_messages(1 - par), field_sems(1 - par))

        lax.fori_loop(0, X // 4 - 1, second_inner, 0)

        @pl.when(m < rounds - 1)
        def _():
            pack_yz()
            send(yz_messages(1 - par), field_sems(1 - par))

        return 0

    lax.fori_loop(0, rounds, step_pair, 0)
    await_sent(cx_messages() + cx_forwards() + cyz_messages(), coef_sems)
    result = pltpu.make_async_copy(F.at[pl.ds(2, X), pl.ds(8, Y)], out, out_sem)
    result.start()
    result.wait()


def body(sizes, concentration, speed, signs, diffusivity, shear):
    X, Y, Z = concentration.shape
    f32, vmem, dma = jnp.float32, pltpu.VMEM, pltpu.SemaphoreType.DMA
    hbm = pl.BlockSpec(memory_space=pl.ANY)

    def call(q, r, *arrays):
        return pl.pallas_call(
            functools.partial(kernel, q, sizes),
            out_shape=jax.ShapeDtypeStruct((X, Y, Z), f32),
            in_specs=[pl.BlockSpec(memory_space=pltpu.SMEM)] + [hbm] * 4,
            out_specs=hbm,
            scratch_shapes=[
                vmem((X + 4, Y + 24, Z), f32),
                vmem((X + 4, Y + 24, Z), f32),
                vmem((X + 4, Y + 24, Z), f32),
                vmem((X + 4, Y + 24, Z), f32),
                vmem(((X + 2) * Y // 8, 7, 8, Z), f32),
                vmem((X * Y // 8, 7, 8, Z), f32),
                vmem((2, 7, X, Z), f32),
                vmem((4, X * Y + 8, Z), f32),
                vmem((3, X * Y + 8, Z), f32),
                vmem((3, X * Y + 8, Z), jnp.int32),
                vmem((2, 2, 2, 144, Z), f32),
                vmem((2, 2, 144, Z), f32),
                vmem((2, 144, Z), f32),
                vmem((2, 8, Z), f32),
                vmem((2, 2, 2, 2, 8, Z), f32),
                vmem((2, 2, X, Z), f32),
                vmem((2, 2, 2, X, Z), f32),
                vmem((2, 2, 2, X, Z), f32),
                vmem((4, 8, Z), f32),
                vmem((2, 2, 4, 8, Z), f32),
                vmem((2, 4, 144, Z), f32),
                vmem((2, 4, X, Z), f32),
                vmem((2, 4, X, Z), f32),
                vmem((4, 4, 8, Z), f32),
                vmem((2, 4, 4, 8, Z), f32),
                dma((4,)), dma((22,)), dma((2, 22)), dma((8,)), dma((8,)), dma(()),
            ],
            compiler_params=pltpu.CompilerParams(
                collective_id=q, has_side_effects=True, vmem_limit_bytes=48 << 20),
        )(r, *arrays)

    offset = lax.rem(shear[0], sizes[1] * Y)
    branches = [functools.partial(call, q) for q in range(sizes[1])]
    return lax.switch(offset // Y, branches, (offset % Y)[None], concentration,
                      speed.reshape(3, X * Y, Z), signs.reshape(3, X * Y, Z), diffusivity.reshape(X * Y, Z))


def solution(mesh):
    sizes = tuple(mesh.shape[name] for name in ("gx", "gy", "gz"))
    placed = (
        P("gx", "gy", "gz"),
        P(None, "gx", "gy", "gz"),
        P(None, "gx", "gy", "gz"),
        P("gx", "gy", "gz"),
        P(),
    )
    return jax.shard_map(
        functools.partial(body, sizes), mesh=mesh, in_specs=placed, out_specs=P("gx", "gy", "gz"), check_vma=False
    )
```
